128 devices in a mesh: scen: 32 (over x, y, core), own: 4 (over z).
Axes of the slice: x: 4, y: 4, z: 4, core: 2. Of those that a mesh axis runs over, the one named last changes fastest.
Arguments:
- returns: float32 [32768, 4096], P('scen', 'own'), may hold values from -50 to 50, as said below
Outputs:
- shrunk_cov: float32 [4096, 4096], P('scen', 'own')
The draws below stay inside these ranges and needn't reach their ends.
Inputs may be any that keep to these rules, and one draw needn't show every extreme that they name: Finite real returns.
All inputs are finite; a program needn't handle non-finite values.
Results may differ from the reference program's by a relative error of at most 0.00014.
Values sent between devices are 32-bit elements; how exact they have to be, the bound alone decides.
No kernel may reach another device: no remote copies, remote signals or barrier semaphores. Data moves between devices by JAX's collectives and lax.ppermute only.
A program may use at most 128 MiB of HBM per device.

```python
import jax
import jax.numpy as jnp
from jax import lax

P_SIZE = 4096
SCENARIOS = 32768


def draw_returns(key, part):
    keys = jax.random.split(key, 6)
    factor_pos = jnp.arange(P_SIZE, dtype=jnp.float32) / P_SIZE
    scen_pos = jnp.arange(SCENARIOS, dtype=jnp.float32) / SCENARIOS
    col_jitter = jax.random.uniform(keys[0], (P_SIZE,), jnp.float32)
    row_jitter = jax.random.uniform(keys[1], (SCENARIOS,), jnp.float32)
    col_scale = 0.1 * 10.0 ** (factor_pos + 0.3 * (col_jitter - 0.5))
    row_scale = 4.0 ** scen_pos * jnp.exp(0.2 * (row_jitter - 0.5))
    noise = jax.random.normal(keys[2], (SCENARIOS, P_SIZE), jnp.float32)
    offsets = 0.5 * col_scale * jax.random.normal(keys[5], (P_SIZE,), jnp.float32)
    values = row_scale[:, None] * col_scale[None, :] * noise + offsets[None, :]
    return jnp.clip(values, -50.0, 50.0).astype(jnp.float32)


def setup_inputs(seed: int = 0) -> dict:
    seeds = jax.random.split(jax.random.key(seed), 2)
    returns = draw_returns(jax.random.fold_in(seeds[1], 71), 0)
    return dict(returns=returns)


epsilon = 1e-6


def reference(returns):
    scenarios = returns.shape[0]
    order = returns.shape[1]
    col_mean = jnp.sum(returns, axis=0) / scenarios
    centered = returns - col_mean
    gram = lax.dot_general(centered, centered, (((0,), (0,)), ((), ())), precision=lax.Precision.HIGHEST, preferred_element_type=jnp.float32)
    covariance = gram / scenarios
    squares = centered * centered
    trace_sum = jnp.sum(squares)
    row_norm = jnp.sum(squares, axis=1)
    beta_raw = jnp.sum(row_norm * row_norm)
    frob_sum = jnp.sum(covariance * covariance)
    target = trace_sum / (scenarios * order)
    beta_term = (beta_raw / scenarios - frob_sum) / (order * scenarios)
    delta_term = (frob_sum - order * target * target) / order
    shrinkage = beta_term / (delta_term + epsilon)
    row_ids = lax.broadcasted_iota(jnp.int32, (order, order), 0)
    col_ids = lax.broadcasted_iota(jnp.int32, (order, order), 1)
    diag_mask = (row_ids == col_ids).astype(jnp.float32)
    return (1.0 - shrinkage) * covariance + shrinkage * target * diag_mask
```

```python
import functools

import jax
import jax.numpy as jnp
from jax import lax
from jax.experimental import pallas as pl
from jax.experimental.pallas import tpu as pltpu
from jax.sharding import Mesh
from jax.sharding import PartitionSpec as P


AXES = ("x", "y", "c", "z")
SCEN = ("x", "y", "c")
EPS = 1e-06
VMEM = 20 * 2**20


def routes(move):
    pairs = []
    for x in range(4):
        for y in range(4):
            for c in range(2):
                for z in range(4):
                    a, b, d, e = move(x, y, c, z)
                    pairs.append((((x * 4 + y) * 2 + c) * 4 + z, ((a * 4 + b) * 2 + d) * 4 + e % 4))
    return pairs


def side(c):
    return 1 if c == 0 else 3


TO_Z = routes(lambda x, y, c, z: (x, y, c, z - side(c)))
OTHER_CORE = routes(lambda x, y, c, z: (x, y, 1 - c, z))
FLIP_NEAR = [
    routes(lambda x, y, c, z, f=f: (y, x, c if f == 0 else 1 - c, z + side(c))) for f in (0, 1)
]
FLIP_FAR = [routes(lambda x, y, c, z, f=f: (y, x, c if f == 0 else 1 - c, z + 2)) for f in (0, 1)]
ACROSS = routes(lambda x, y, c, z: (x, y, c, z + 2))
X_BY = {d: routes(lambda x, y, c, z, d=d: (x ^ d, y, c, z)) for d in (1, 2, 3)}
X_HALF = [routes(lambda x, y, c, z, f=f: (x ^ (1 if c == f else 3), y, c, z)) for f in (0, 1)]
Y_HALF = [routes(lambda x, y, c, z, f=f: (x, y ^ (1 if c == f else 3), c, z)) for f in (0, 1)]


def send(a, route):
    return lax.ppermute(a, AXES, route)


def to_everyone(a, axes):
    copies = jnp.broadcast_to(a, (lax.axis_size(axes), *a.shape))
    return lax.all_to_all(copies, axes, split_axis=0, concat_axis=0, tiled=True)


def swapped(k):
    return jnp.where(k == 1, 2, jnp.where(k == 2, 1, k))


def high_low(a):
    high = a.astype(jnp.bfloat16)
    return high, (a - high.astype(jnp.float32)).astype(jnp.bfloat16)


def prepare_body(at_ref, a_ref, mean_ref, high_ref, low_ref):
    g = a_ref.shape[1] // 8
    for j in range(8):
        cols = pl.ds(pl.multiple_of(at_ref[j] * g, g), g)
        to = slice(j * g, (j + 1) * g)
        high_ref[:, to], low_ref[:, to] = high_low(a_ref[:, cols] - mean_ref[:, cols])


def prepare(a, mean, at):
    k, n = a.shape
    out = jax.ShapeDtypeStruct((k, n), jnp.bfloat16)
    spec = pl.BlockSpec((k // 8, n), lambda j, at: (j, 0))
    return pl.pallas_call(
        prepare_body,
        grid_spec=pltpu.PrefetchScalarGridSpec(
            num_scalar_prefetch=1,
            grid=(8,),
            in_specs=[spec, pl.BlockSpec((1, n), lambda j, at: (0, 0))],
            out_specs=[spec, spec],
        ),
        out_shape=[out, out],
        compiler_params=pltpu.CompilerParams(vmem_limit_bytes=VMEM),
        name="prepare",
    )(at, a, mean)


def gram_body(at_ref, mean_ref, *refs, terms, extra):
    k = pl.program_id(0)
    ins, refs = refs[: 3 * terms], refs[3 * terms :]
    if extra:
        sums, refs = refs[:4], refs[4:]
    norms, outs = refs[:terms], refs[terms:]
    dims = (((0,), (0,)), ((), ()))
    dot = lambda l, r: lax.dot_general(l, r, dims, preferred_element_type=jnp.float32)
    total = None
    for t in range(terms):
        a_ref, high_ref, low_ref = ins[3 * t : 3 * t + 3]
        a = a_ref[...] - mean_ref[...]
        norm = jnp.sum(a * a, axis=1, keepdims=True)

        @pl.when(k == 0)
        def _():
            norms[t][...] = norm

        @pl.when(k > 0)
        def _():
            norms[t][...] += norm

        high, low = high_low(a)
        part = dot(high, high_ref[...]) + (dot(high, low_ref[...]) + dot(low, high_ref[...]))
        total = part if total is None else total + part
    g = total.shape[0] // 2
    tile = lambda r, v, q: total[r * g : (r + 1) * g, (2 * v + q) * g : (2 * v + q + 1) * g]
    if extra:
        a_keep, a_away, b_keep, b_away = outs
        for v in range(4):
            ref = b_keep if v < 2 else b_away
            for q in range(2):
                ref[v % 2, 0, q] = tile(1, v, q)
            ref[v % 2, 0, 2] = sums[2][v, 0] + sums[3][v, 0]

        def put(ref):
            for v in range(4):
                for q in range(2):
                    ref[0, v, q] = tile(0, v, q)
                ref[0, v, 2] = sums[0][0, v] + sums[1][0, v]

        @pl.when(k < 2)
        def _():
            put(a_keep)

        @pl.when(k >= 2)
        def _():
            put(a_away)
    else:
        a_all, b_all, a_over, b_over = outs
        for v in range(4):
            w = (0, 2, 1, 3)[v]
            a_all[0, v] = tile(0, v, 0)
            b_all[v, 0] = tile(1, v, 1)
            a_over[0, w] = tile(0, v, 1)
            b_over[w, 0] = tile(1, v, 0)


def gram(lefts, mean, right, at, sums):
    terms = len(lefts)
    high, low = right
    n = high.shape[1]
    h = high.shape[0] // 2
    g = n // 8
    specs = [pl.BlockSpec((1, 2 * g), lambda k, at: (0, at[k]))]
    args = [mean]
    for t, left in enumerate(lefts):
        specs.append(pl.BlockSpec((h, 2 * g), lambda k, at, t=t: (at[4 + 2 * t], at[k])))
        row = pl.BlockSpec(
            (h, n), lambda k, at, t=t: (at[5 + 2 * t], 0), pipeline_mode=pl.Buffered(1)
        )
        specs += [row, row]
        args += [left, high, low]
    in_row = pl.BlockSpec((1, 4, g, g), lambda k, at: (k, 0, 0, 0))
    in_col = pl.BlockSpec((4, 1, g, g), lambda k, at: (0, k, 0, 0))
    shapes = [(h, 1)] * terms
    outs = [pl.BlockSpec((h, 1), lambda k, at: (0, 0))] * terms
    if sums:
        specs += [in_row, in_row, in_col, in_col]
        args += sums
        shapes += [(2, 4, 3, g, g)] * 4
        outs += [
            pl.BlockSpec((1, 4, 3, g, g), lambda k, at: (jnp.minimum(k, 1), 0, 0, 0, 0)),
            pl.BlockSpec((1, 4, 3, g, g), lambda k, at: (jnp.maximum(k - 2, 0), 0, 0, 0, 0)),
        ] + [pl.BlockSpec((2, 1, 3, g, g), lambda k, at: (0, k, 0, 0, 0))] * 2
    else:
        shapes += [(4, 4, g, g)] * 4
        outs += [
            in_row,
            in_col,
            pl.BlockSpec((1, 4, g, g), lambda k, at: (swapped(k), 0, 0, 0)),
            pl.BlockSpec((4, 1, g, g), lambda k, at: (0, swapped(k), 0, 0)),
        ]
    res = pl.pallas_call(
        functools.partial(gram_body, terms=terms, extra=bool(sums)),
        grid_spec=pltpu.PrefetchScalarGridSpec(
            num_scalar_prefetch=1, grid=(4,), in_specs=specs, out_specs=outs
        ),
        out_shape=[jax.ShapeDtypeStruct(i, jnp.float32) for i in shapes],
        cost_estimate=pl.CostEstimate(
            flops=6 * terms * h * n * n, bytes_accessed=8 * n * n, transcendentals=0
        ),
        compiler_params=pltpu.CompilerParams(vmem_limit_bytes=VMEM),
    )(at, *args)
    return res[:terms], res[terms:]


def flip_body(a_ref, out_ref):
    for i in range(a_ref.shape[0]):
        out_ref[i] = a_ref[i].T


def flip(a):
    return pl.pallas_call(
        flip_body,
        out_shape=jax.ShapeDtypeStruct(a.shape, jnp.float32),
        compiler_params=pltpu.CompilerParams(vmem_limit_bytes=VMEM),
        name="flip",
    )(a)


def combine_body(
    at_ref, pa, pb, qa, qb, d_got, p_got, q_got, p_own, p_other, q_left, q_right,
    norm0, norm1, near0, near1, far0, own_ref, out1, out2, out3, sums_ref, blocks,
    *, scenarios,
):
    c, e, h = at_ref[0], at_ref[1], at_ref[2]
    first = c == 0
    mine = lambda a, b: jnp.where(first, a, b)
    g = qa.shape[0]
    own = [mine(pa[i], pb[1 - i]) + p_own[i] for i in range(2)]
    other = [mine(p_got[1 - i], p_got[i]) + p_other[i] for i in range(2)]
    left = [
        mine(pa[2], pb[2]),
        mine(own[0], other[0]),
        mine(qa[...], qb[...]) + q_left[...],
        mine(other[0], own[0]),
    ]
    right = [
        d_got[...],
        mine(own[1], other[1]),
        q_got[...] + q_right[...],
        mine(other[1], own[1]),
    ]
    squares = None
    for i in range(4):
        for j, a in enumerate((left[i], right[i])):
            a = a * (1.0 / scenarios)
            blocks[i, :, j * g : (j + 1) * g] = a
            squares = a * a if squares is None else squares + a * a
    all_of = lambda a: jnp.sum(jnp.sum(a, axis=1, keepdims=True), axis=0, keepdims=True)
    frob = all_of(squares)
    n0, n1, m0, m1 = norm0[...], norm1[...], near0[...], near1[...]
    straight = n0 * m0 + n1 * m1
    crossed = n0 * m1 + n1 * m0
    far = jnp.where(h == 0, n0, n1) * far0[...]
    beta = all_of(n0 * n0 + n1 * n1 + 2.0 * (jnp.where(e == 0, straight, crossed) + far))
    trace = all_of(n0 + n1)
    lane = lax.broadcasted_iota(jnp.int32, (1, 128), 1)
    row = jnp.where(lane == 0, trace, jnp.where(lane == 1, beta, jnp.where(lane == 2, frob, 0.0)))
    sums_ref[...] = jnp.broadcast_to(row.reshape(1, 1, 128), sums_ref.shape)
    for i, ref in enumerate((own_ref, out1, out2, out3)):
        ref[...] = blocks[at_ref[3 + i]]


def combine(at, arrays, scenarios):
    g = arrays[2].shape[0]
    tile = jax.ShapeDtypeStruct((g, 2 * g), jnp.float32)
    return pl.pallas_call(
        functools.partial(combine_body, scenarios=scenarios),
        in_specs=[pl.BlockSpec(memory_space=pltpu.SMEM)]
        + [pl.BlockSpec(memory_space=pltpu.VMEM)] * len(arrays),
        out_shape=[tile] * 4 + [jax.ShapeDtypeStruct((128, 1, 128), jnp.float32)],
        scratch_shapes=[pltpu.VMEM((4, g, 2 * g), jnp.float32)],
        compiler_params=pltpu.CompilerParams(vmem_limit_bytes=VMEM),
        name="combine",
    )(at, *arrays)


def shrink_body(at_ref, own, got1, got2, got3, sums_ref, out_ref, *, scenarios, order):
    sums = jnp.sum(sums_ref[...], axis=0)
    lane = lax.broadcasted_iota(jnp.int32, sums.shape, 1)
    one = lambda i: jnp.sum(jnp.where(lane == i, sums, 0.0), axis=1, keepdims=True)
    trace_sum, beta_raw, frob_sum = one(0), one(1), one(2)
    target = trace_sum / (scenarios * order)
    beta_term = (beta_raw / scenarios - frob_sum) / (order * scenarios)
    delta_term = (frob_sum - order * target * target) / order
    shrinkage = beta_term / (delta_term + EPS)
    keep, add = 1.0 - shrinkage, shrinkage * target
    g, w = own.shape
    rows = lax.broadcasted_iota(jnp.int32, (g, w), 0)
    cols = lax.broadcasted_iota(jnp.int32, (g, w), 1)
    for i, ref in enumerate((own, got1, got2, got3)):
        at = at_ref[i]
        on = rows + at_ref[4] == cols + at * w
        to = pl.ds(pl.multiple_of(at * w, w), w)
        out_ref[:, to] = keep * ref[...] + jnp.where(on, add, 0.0)


def shrink(at, arrays, scenarios, order):
    g, w = arrays[0].shape
    return pl.pallas_call(
        functools.partial(shrink_body, scenarios=scenarios, order=order),
        in_specs=[pl.BlockSpec(memory_space=pltpu.SMEM)]
        + [pl.BlockSpec(memory_space=pltpu.VMEM)] * len(arrays),
        out_shape=jax.ShapeDtypeStruct((g, 4 * w), jnp.float32),
        compiler_params=pltpu.CompilerParams(vmem_limit_bytes=VMEM),
        name="shrink",
    )(at, *arrays)


def halve(keep, away, routes_of):
    total = keep + send(away, routes_of[0])
    return total[0] + send(total[1], routes_of[1])


def finish(parts):
    a = halve(parts[0], parts[1], Y_HALF)
    b = halve(parts[2], parts[3], X_HALF)
    a = halve(a[:2], a[2:], X_HALF)
    return a, halve(b[:2], b[2:], Y_HALF)


def from_core(parts):
    return [send(parts[2 + i], OTHER_CORE) for i in range(2)]


def on_device(returns):
    local, n = returns.shape
    g = n // 8
    half = local // 2
    scenarios = local * 32
    order = n * 4
    x, y, c, z = (lax.axis_index(a) for a in AXES)
    first = c == 0
    low_z = (z < 2).astype(jnp.int32)
    early_raw = send(lax.dynamic_slice_in_dim(returns, low_z * half, half), TO_Z)
    late_raw = send(lax.dynamic_slice_in_dim(returns, (1 - low_z) * half, half), TO_Z)
    far_raw = send(early_raw, TO_Z)
    sums = to_everyone(jnp.sum(returns, axis=0, keepdims=True), SCEN)
    mean = jnp.sum(sums, axis=0).reshape(1, n) / scenarios
    mean_near = send(mean, TO_Z)
    mean_far = send(mean, ACROSS)

    turn = [jnp.where(first, i, j) for i, j in ((0, 0), (3, 1), (1, 3), (2, 2))]
    ys = [y ^ i for i in turn]
    cols = [2 * (x ^ i) + k for i in turn for k in (c, 1 - c)]
    right = prepare(returns, mean, jnp.stack(cols))
    near_z = (z + jnp.where(first, 1, 3)) % 4
    near_early = (near_z < 2).astype(jnp.int32)
    far_half = 1 - low_z
    (norm0, norm1), d_parts = gram(
        [returns, returns], mean, right, jnp.stack(ys + [0, 0, 1, 1]), None
    )
    d_over = from_core(d_parts)
    (near0, near1), p_parts = gram(
        [early_raw, late_raw],
        mean_near,
        right,
        jnp.stack(ys + [0, near_early, 0, 1 - near_early]),
        [d_parts[0], d_over[0], d_parts[1], d_over[1]],
    )
    pa, pb = finish(p_parts)
    (far0,), q_parts = gram([far_raw], mean_far, right, jnp.stack(ys + [0, far_half]), None)
    q_over = from_core(q_parts)
    q_keep = [q_parts[i][:2] + q_over[i][:2] for i in range(2)]
    q_away = [q_parts[i][2:] + q_over[i][2:] for i in range(2)]
    q = finish([q_keep[0], q_away[0], q_keep[1], q_away[1]])

    mine = lambda a, b: jnp.where(first, a, b)
    d_got = send(mine(pb[2], pa[2]), OTHER_CORE)
    p_got = send(mine(pb[:2], pa[:2]), OTHER_CORE)
    p_flip = flip(jnp.stack([pa[0], pb[0], pa[1], pb[1]]))
    p_other = send(p_flip[:2], FLIP_NEAR[0])
    p_own = send(p_flip[2:], FLIP_NEAR[1])
    q_got = send(mine(q[1], q[0]), OTHER_CORE)
    q_flip = flip(jnp.stack(q))
    q_left = send(q_flip[0], FLIP_FAR[0])
    q_right = send(q_flip[1], FLIP_FAR[1])
    at = jnp.stack([c, near_early, far_half] + [((x ^ i) - z) % 4 for i in range(4)])
    *tiles, sums = combine(
        at,
        [pa, pb, q[0], q[1], d_got, p_got, q_got, p_own, p_other, q_left, q_right]
        + [norm0, norm1, near0, near1, far0],
        scenarios,
    )
    tiles = [tiles[0]] + [send(tiles[i], X_BY[i]) for i in (1, 2, 3)]
    sums = lax.all_to_all(sums, AXES, split_axis=0, concat_axis=0, tiled=True)
    row = (x - z) * n + (2 * y + c) * g
    at = jnp.stack([x, x ^ 1, x ^ 2, x ^ 3, row])
    return shrink(at, tiles + [sums], scenarios, order)


def solution(mesh):
    torus = Mesh(mesh.devices.reshape(4, 4, 2, 4), AXES)
    spec = P(SCEN, "z")

    return jax.shard_map(on_device, mesh=torus, in_specs=(spec,), out_specs=spec, check_vma=False)
```

```python
import functools

import jax
import jax.numpy as jnp
from jax import lax
from jax.experimental import pallas as pl
from jax.experimental.pallas import tpu as pltpu
from jax.sharding import Mesh
from jax.sharding import PartitionSpec as P


AXES = ("x", "y", "c", "z")
SCEN = ("x", "y", "c")
EPS = 1e-06
VMEM = 20 * 2**20
VMEM_LATE = 56 * 2**20


def routes(move):
    pairs = []
    for x in range(4):
        for y in range(4):
            for c in range(2):
                for z in range(4):
                    a, b, d, e = move(x, y, c, z)
                    pairs.append((((x * 4 + y) * 2 + c) * 4 + z, ((a * 4 + b) * 2 + d) * 4 + e % 4))
    return pairs


def side(c):
    return 1 if c == 0 else 3


TO_Z = routes(lambda x, y, c, z: (x, y, c, z - side(c)))
OTHER_CORE = routes(lambda x, y, c, z: (x, y, 1 - c, z))
FLIP_NEAR = [
    routes(lambda x, y, c, z, f=f: (y, x, c if f == 0 else 1 - c, z + side(c))) for f in (0, 1)
]
FLIP_FAR = [routes(lambda x, y, c, z, f=f: (y, x, c if f == 0 else 1 - c, z + 2)) for f in (0, 1)]
ACROSS = routes(lambda x, y, c, z: (x, y, c, z + 2))
X_BY = {d: routes(lambda x, y, c, z, d=d: (x ^ d, y, c, z)) for d in (1, 2, 3)}
X_HALF = [routes(lambda x, y, c, z, f=f: (x ^ (1 if c == f else 3), y, c, z)) for f in (0, 1)]
Y_HALF = [routes(lambda x, y, c, z, f=f: (x, y ^ (1 if c == f else 3), c, z)) for f in (0, 1)]


def send(a, route):
    return lax.ppermute(a, AXES, route)


def to_everyone(a, axes):
    copies = jnp.broadcast_to(a, (lax.axis_size(axes), *a.shape))
    return lax.all_to_all(copies, axes, split_axis=0, concat_axis=0, tiled=True)


def swapped(k):
    return jnp.where(k == 1, 2, jnp.where(k == 2, 1, k))


def high_low(a):
    high = a.astype(jnp.bfloat16)
    return high, (a - high.astype(jnp.float32)).astype(jnp.bfloat16)


def prepare_body(at_ref, a_ref, mean_ref, high_ref, low_ref):
    g = a_ref.shape[1] // 8
    for j in range(8):
        cols = pl.ds(pl.multiple_of(at_ref[j] * g, g), g)
        to = slice(j * g, (j + 1) * g)
        high_ref[:, to], low_ref[:, to] = high_low(a_ref[:, cols] - mean_ref[:, cols])


def prepare(a, mean, at):
    k, n = a.shape
    out = jax.ShapeDtypeStruct((k, n), jnp.bfloat16)
    spec = pl.BlockSpec((k // 8, n), lambda j, at: (j, 0))
    return pl.pallas_call(
        prepare_body,
        grid_spec=pltpu.PrefetchScalarGridSpec(
            num_scalar_prefetch=1,
            grid=(8,),
            in_specs=[spec, pl.BlockSpec((1, n), lambda j, at: (0, 0))],
            out_specs=[spec, spec],
        ),
        out_shape=[out, out],
        compiler_params=pltpu.CompilerParams(vmem_limit_bytes=VMEM),
        name="prepare",
    )(at, a, mean)


def gram_body(at_ref, mean_ref, *refs, terms, extra):
    k = pl.program_id(0)
    ins, refs = refs[: 3 * terms], refs[3 * terms :]
    if extra:
        sums, refs = refs[:4], refs[4:]
    norms, outs = refs[:terms], refs[terms:]
    dims = (((0,), (0,)), ((), ()))
    dot = lambda l, r: lax.dot_general(l, r, dims, preferred_element_type=jnp.float32)
    total = None
    for t in range(terms):
        a_ref, high_ref, low_ref = ins[3 * t : 3 * t + 3]
        a = a_ref[...] - mean_ref[...]
        norm = jnp.sum(a * a, axis=1, keepdims=True)

        @pl.when(k == 0)
        def _():
            norms[t][...] = norm

        @pl.when(k > 0)
        def _():
            norms[t][...] += norm

        high, low = high_low(a)
        part = dot(high, high_ref[...]) + (dot(high, low_ref[...]) + dot(low, high_ref[...]))
        total = part if total is None else total + part
    g = total.shape[0] // 2
    tile = lambda r, v, q: total[r * g : (r + 1) * g, (2 * v + q) * g : (2 * v + q + 1) * g]
    if extra:
        a_keep, a_away, b_keep, b_away = outs
        for v in range(4):
            ref = b_keep if v < 2 else b_away
            for q in range(2):
                ref[v % 2, 0, q] = tile(1, v, q)
            ref[v % 2, 0, 2] = sums[2][v, 0] + sums[3][v, 0]

        def put(ref):
            for v in range(4):
                for q in range(2):
                    ref[0, v, q] = tile(0, v, q)
                ref[0, v, 2] = sums[0][0, v] + sums[1][0, v]

        @pl.when(k < 2)
        def _():
            put(a_keep)

        @pl.when(k >= 2)
        def _():
            put(a_away)
    else:
        a_all, b_all, a_over, b_over = outs
        for v in range(4):
            w = (0, 2, 1, 3)[v]
            a_all[0, v] = tile(0, v, 0)
            b_all[v, 0] = tile(1, v, 1)
            a_over[0, w] = tile(0, v, 1)
            b_over[w, 0] = tile(1, v, 0)


def gram(lefts, mean, right, at, sums, vmem):
    terms = len(lefts)
    high, low = right
    n = high.shape[1]
    h = high.shape[0] // 2
    g = n // 8
    specs = [pl.BlockSpec((1, 2 * g), lambda k, at: (0, at[k]))]
    args = [mean]
    for t, left in enumerate(lefts):
        specs.append(pl.BlockSpec((h, 2 * g), lambda k, at, t=t: (at[4 + 2 * t], at[k])))
        row = pl.BlockSpec(
            (h, n), lambda k, at, t=t: (at[5 + 2 * t], 0), pipeline_mode=pl.Buffered(1)
        )
        specs += [row, row]
        args += [left, high, low]
    in_row = pl.BlockSpec((1, 4, g, g), lambda k, at: (k, 0, 0, 0))
    in_col = pl.BlockSpec((4, 1, g, g), lambda k, at: (0, k, 0, 0))
    shapes = [(h, 1)] * terms
    outs = [pl.BlockSpec((h, 1), lambda k, at: (0, 0))] * terms
    if sums:
        specs += [in_row, in_row, in_col, in_col]
        args += sums
        shapes += [(2, 4, 3, g, g)] * 4
        outs += [
            pl.BlockSpec((1, 4, 3, g, g), lambda k, at: (jnp.minimum(k, 1), 0, 0, 0, 0)),
            pl.BlockSpec((1, 4, 3, g, g), lambda k, at: (jnp.maximum(k - 2, 0), 0, 0, 0, 0)),
        ] + [pl.BlockSpec((2, 1, 3, g, g), lambda k, at: (0, k, 0, 0, 0))] * 2
    else:
        shapes += [(4, 4, g, g)] * 4
        outs += [
            in_row,
            in_col,
            pl.BlockSpec((1, 4, g, g), lambda k, at: (swapped(k), 0, 0, 0)),
            pl.BlockSpec((4, 1, g, g), lambda k, at: (0, swapped(k), 0, 0)),
        ]
    res = pl.pallas_call(
        functools.partial(gram_body, terms=terms, extra=bool(sums)),
        grid_spec=pltpu.PrefetchScalarGridSpec(
            num_scalar_prefetch=1, grid=(4,), in_specs=specs, out_specs=outs
        ),
        out_shape=[jax.ShapeDtypeStruct(i, jnp.float32) for i in shapes],
        cost_estimate=pl.CostEstimate(
            flops=6 * terms * h * n * n, bytes_accessed=8 * n * n, transcendentals=0
        ),
        compiler_params=pltpu.CompilerParams(vmem_limit_bytes=vmem),
    )(at, *args)
    return res[:terms], res[terms:]


def flip_body(a_ref, out_ref):
    for i in range(a_ref.shape[0]):
        out_ref[i] = a_ref[i].T


def flip(a):
    return pl.pallas_call(
        flip_body,
        out_shape=jax.ShapeDtypeStruct(a.shape, jnp.float32),
        compiler_params=pltpu.CompilerParams(vmem_limit_bytes=VMEM),
        name="flip",
    )(a)


def combine_body(
    at_ref, pa, pb, qa, qb, got, p_own, p_other, q_left, q_right,
    norm0, norm1, near0, near1, far0, own_ref, out1, out2, out3, sums_ref, blocks,
    *, scenarios,
):
    c, h = at_ref[0], at_ref[1]
    first = c == 0
    mine = lambda a, b: jnp.where(first, a, b)
    g = qa.shape[0]
    own = [mine(pa[i], pb[1 - i]) + p_own[i] for i in range(2)]
    other = [mine(got[1 - i], got[i]) + p_other[i] for i in range(2)]
    left = [
        mine(pa[2], pb[2]),
        mine(own[0], other[0]),
        mine(qa[...], qb[...]) + q_left[...],
        mine(other[0], own[0]),
    ]
    right = [
        got[2],
        mine(own[1], other[1]),
        got[3] + q_right[...],
        mine(other[1], own[1]),
    ]
    squares = None
    for i in range(4):
        for j, a in enumerate((left[i], right[i])):
            a = a * (1.0 / scenarios)
            blocks[i, :, j * g : (j + 1) * g] = a
            squares = a * a if squares is None else squares + a * a
    all_of = lambda a: jnp.sum(jnp.sum(a, axis=1, keepdims=True), axis=0, keepdims=True)
    frob = all_of(squares)
    n0, n1, m0, m1 = norm0[...], norm1[...], near0[...], near1[...]
    near = n0 * m0 + n1 * m1
    far = jnp.where(h == 0, n0, n1) * far0[...]
    beta = all_of(n0 * n0 + n1 * n1 + 2.0 * (near + far))
    trace = all_of(n0 + n1)
    lane = lax.broadcasted_iota(jnp.int32, (1, 128), 1)
    row = jnp.where(lane == 0, trace, jnp.where(lane == 1, beta, jnp.where(lane == 2, frob, 0.0)))
    sums_ref[...] = jnp.broadcast_to(row.reshape(1, 1, 128), sums_ref.shape)
    for i, ref in enumerate((own_ref, out1, out2, out3)):
        ref[...] = blocks[at_ref[2 + i]]


def combine(at, arrays, scenarios):
    g = arrays[2].shape[0]
    tile = jax.ShapeDtypeStruct((g, 2 * g), jnp.float32)
    return pl.pallas_call(
        functools.partial(combine_body, scenarios=scenarios),
        in_specs=[pl.BlockSpec(memory_space=pltpu.SMEM)]
        + [pl.BlockSpec(memory_space=pltpu.VMEM)] * len(arrays),
        out_shape=[tile] * 4 + [jax.ShapeDtypeStruct((128, 1, 128), jnp.float32)],
        scratch_shapes=[pltpu.VMEM((4, g, 2 * g), jnp.float32)],
        compiler_params=pltpu.CompilerParams(vmem_limit_bytes=VMEM),
        name="combine",
    )(at, *arrays)


def shrink_body(at_ref, own, got1, got2, got3, sums_ref, out_ref, *, scenarios, order):
    sums = jnp.sum(sums_ref[...], axis=0)
    lane = lax.broadcasted_iota(jnp.int32, sums.shape, 1)
    one = lambda i: jnp.sum(jnp.where(lane == i, sums, 0.0), axis=1, keepdims=True)
    trace_sum, beta_raw, frob_sum = one(0), one(1), one(2)
    target = trace_sum / (scenarios * order)
    beta_term = (beta_raw / scenarios - frob_sum) / (order * scenarios)
    delta_term = (frob_sum - order * target * target) / order
    shrinkage = beta_term / (delta_term + EPS)
    keep, add = 1.0 - shrinkage, shrinkage * target
    g, w = own.shape
    rows = lax.broadcasted_iota(jnp.int32, (g, w), 0)
    cols = lax.broadcasted_iota(jnp.int32, (g, w), 1)
    for i, ref in enumerate((own, got1, got2, got3)):
        at = at_ref[i]
        on = rows + at_ref[4] == cols + at * w
        to = pl.ds(pl.multiple_of(at * w, w), w)
        out_ref[:, to] = keep * ref[...] + jnp.where(on, add, 0.0)


def shrink(at, arrays, scenarios, order):
    g, w = arrays[0].shape
    return pl.pallas_call(
        functools.partial(shrink_body, scenarios=scenarios, order=order),
        in_specs=[pl.BlockSpec(memory_space=pltpu.SMEM)]
        + [pl.BlockSpec(memory_space=pltpu.VMEM)] * len(arrays),
        out_shape=jax.ShapeDtypeStruct((g, 4 * w), jnp.float32),
        compiler_params=pltpu.CompilerParams(vmem_limit_bytes=VMEM),
        name="shrink",
    )(at, *arrays)


def halve(keep, away, routes_of):
    got = send(away, routes_of[0])
    total = keep + got
    return total[0] + send(total[1], routes_of[1])


def finish(parts):
    a = halve(parts[0], parts[1], Y_HALF)
    b = halve(parts[2], parts[3], X_HALF)
    a = halve(a[:2], a[2:], X_HALF)
    return a, halve(b[:2], b[2:], Y_HALF)


def from_core(parts):
    return [send(parts[2 + i], OTHER_CORE) for i in range(2)]


def on_device(returns):
    local, n = returns.shape
    g = n // 8
    half = local // 2
    scenarios = local * 32
    order = n * 4
    x, y, c, z = (lax.axis_index(a) for a in AXES)
    first = c == 0
    near_raw = send(returns, TO_Z)
    sums = to_everyone(jnp.sum(returns, axis=0, keepdims=True), SCEN)
    mean = jnp.sum(sums, axis=0).reshape(1, n) / scenarios
    mean_near = send(mean, TO_Z)
    mean_far = send(mean, ACROSS)

    turn = [jnp.where(first, i, j) for i, j in ((0, 0), (3, 1), (1, 3), (2, 2))]
    ys = [y ^ i for i in turn]
    cols = [2 * (x ^ i) + k for i in turn for k in (c, 1 - c)]
    right = prepare(returns, mean, jnp.stack(cols))
    far_half = (z >= 2).astype(jnp.int32)
    ahead = (z + jnp.where(first, 3, 1)) % 4
    far_raw = send(lax.dynamic_slice_in_dim(near_raw, jnp.where(ahead >= 2, half, 0), half), TO_Z)
    (norm0, norm1), d_parts = gram(
        [returns, returns], mean, right, jnp.stack(ys + [0, 0, 1, 1]), None, VMEM
    )
    d_over = from_core(d_parts)
    (near0, near1), p_parts = gram(
        [near_raw, near_raw],
        mean_near,
        right,
        jnp.stack(ys + [0, 0, 1, 1]),
        [d_parts[0], d_over[0], d_parts[1], d_over[1]],
        VMEM_LATE,
    )
    pa, pb = finish(p_parts)
    (far0,), q_parts = gram(
        [far_raw], mean_far, right, jnp.stack(ys + [0, far_half]), None, VMEM_LATE
    )
    q_over = from_core(q_parts)
    q_keep = [q_parts[i][:2] + q_over[i][:2] for i in range(2)]
    q_away = [q_parts[i][2:] + q_over[i][2:] for i in range(2)]
    q = finish([q_keep[0], q_away[0], q_keep[1], q_away[1]])

    mine = lambda a, b: jnp.where(first, a, b)
    p_flip = flip(jnp.stack([pa[0], pb[0], pa[1], pb[1]]))
    p_other = send(p_flip[:2], FLIP_NEAR[0])
    p_own = send(p_flip[2:], FLIP_NEAR[1])
    got = send(
        mine(jnp.concatenate([pb, q[1][None]]), jnp.concatenate([pa, q[0][None]])), OTHER_CORE
    )
    q_flip = flip(jnp.stack(q))
    q_left = send(q_flip[0], FLIP_FAR[0])
    q_right = send(q_flip[1], FLIP_FAR[1])
    at = jnp.stack([c, far_half] + [((x ^ i) - z) % 4 for i in range(4)])
    *tiles, sums = combine(
        at,
        [pa, pb, q[0], q[1], got, p_own, p_other, q_left, q_right]
        + [norm0, norm1, near0, near1, far0],
        scenarios,
    )
    tiles = [tiles[0]] + [send(tiles[i], X_BY[i]) for i in (1, 2, 3)]
    sums = lax.all_to_all(sums, AXES, split_axis=0, concat_axis=0, tiled=True)
    row = (x - z) * n + (2 * y + c) * g
    at = jnp.stack([x, x ^ 1, x ^ 2, x ^ 3, row])
    return shrink(at, tiles + [sums], scenarios, order)


def solution(mesh):
    torus = Mesh(mesh.devices.reshape(4, 4, 2, 4), AXES)
    spec = P(SCEN, "z")

    return jax.shard_map(on_device, mesh=torus, in_specs=(spec,), out_specs=spec, check_vma=False)
```

```python
import functools

import jax
import jax.numpy as jnp
from jax import lax
from jax.experimental import pallas as pl
from jax.experimental.pallas import tpu as pltpu
from jax.sharding import Mesh
from jax.sharding import PartitionSpec as P


AXES = ("x", "y", "c", "z")
SCEN = ("x", "y", "c")
EPS = 1e-06
VMEM = 20 * 2**20
VMEM_LATE = 56 * 2**20


def routes(move):
    pairs = []
    for x in range(4):
        for y in range(4):
            for c in range(2):
                for z in range(4):
                    a, b, d, e = move(x, y, c, z)
                    pairs.append((((x * 4 + y) * 2 + c) * 4 + z, ((a * 4 + b) * 2 + d) * 4 + e % 4))
    return pairs


def side(c):
    return 1 if c == 0 else 3


TO_Z = routes(lambda x, y, c, z: (x, y, c, z - side(c)))
OTHER_CORE = routes(lambda x, y, c, z: (x, y, 1 - c, z))
FLIP_NEAR = [
    routes(lambda x, y, c, z, f=f: (y, x, c if f == 0 else 1 - c, z + side(c))) for f in (0, 1)
]
FLIP_FAR = [routes(lambda x, y, c, z, f=f: (y, x, c if f == 0 else 1 - c, z + 2)) for f in (0, 1)]
ACROSS = routes(lambda x, y, c, z: (x, y, c, z + 2))
X_BY = {d: routes(lambda x, y, c, z, d=d: (x ^ d, y, c, z)) for d in (1, 2, 3)}
X_HALF = [routes(lambda x, y, c, z, f=f: (x ^ (1 if c == f else 3), y, c, z)) for f in (0, 1)]
Y_HALF = [routes(lambda x, y, c, z, f=f: (x, y ^ (1 if c == f else 3), c, z)) for f in (0, 1)]


def send(a, route):
    return lax.ppermute(a, AXES, route)


def to_everyone(a, axes):
    copies = jnp.broadcast_to(a, (lax.axis_size(axes), *a.shape))
    return lax.all_to_all(copies, axes, split_axis=0, concat_axis=0, tiled=True)


def swapped(k):
    return jnp.where(k == 1, 2, jnp.where(k == 2, 1, k))


def high_low(a):
    high = a.astype(jnp.bfloat16)
    return high, (a - high.astype(jnp.float32)).astype(jnp.bfloat16)


def prepare_body(at_ref, a_ref, mean_ref, high_ref, low_ref):
    g = a_ref.shape[1] // 8
    for j in range(8):
        cols = pl.ds(pl.multiple_of(at_ref[j] * g, g), g)
        to = slice(j * g, (j + 1) * g)
        high_ref[:, to], low_ref[:, to] = high_low(a_ref[:, cols] - mean_ref[:, cols])


def prepare(a, mean, at):
    k, n = a.shape
    out = jax.ShapeDtypeStruct((k, n), jnp.bfloat16)
    spec = pl.BlockSpec((k // 8, n), lambda j, at: (j, 0))
    return pl.pallas_call(
        prepare_body,
        grid_spec=pltpu.PrefetchScalarGridSpec(
            num_scalar_prefetch=1,
            grid=(8,),
            in_specs=[spec, pl.BlockSpec((1, n), lambda j, at: (0, 0))],
            out_specs=[spec, spec],
        ),
        out_shape=[out, out],
        compiler_params=pltpu.CompilerParams(vmem_limit_bytes=VMEM),
        name="prepare",
    )(at, a, mean)


def gram_body(at_ref, mean_ref, *refs, terms, extra):
    k = pl.program_id(0)
    ins, refs = refs[: 3 * terms], refs[3 * terms :]
    if extra:
        sums, refs = refs[:4], refs[4:]
    norms, outs = refs[:terms], refs[terms:]
    dims = (((1,), (0,)), ((), ()))
    dot = lambda l, r: lax.dot_general(l, r, dims, preferred_element_type=jnp.float32)
    total = None
    for t in range(terms):
        a_ref, high_ref, low_ref = ins[3 * t : 3 * t + 3]
        a = (a_ref[...] - mean_ref[...]).T
        norm = jnp.sum(a * a, axis=0, keepdims=True)

        @pl.when(k == 0)
        def _():
            norms[t][...] = norm

        @pl.when(k > 0)
        def _():
            norms[t][...] += norm

        high, low = high_low(a)
        part = dot(high, high_ref[...]) + (dot(high, low_ref[...]) + dot(low, high_ref[...]))
        total = part if total is None else total + part
    g = total.shape[0] // 2
    tile = lambda r, v, q: total[r * g : (r + 1) * g, (2 * v + q) * g : (2 * v + q + 1) * g]
    if extra:
        a_keep, a_away, b_keep, b_away = outs
        for v in range(4):
            ref = b_keep if v < 2 else b_away
            for q in range(2):
                ref[v % 2, 0, q] = tile(1, v, q)
            ref[v % 2, 0, 2] = sums[2][v, 0] + sums[3][v, 0]

        def put(ref):
            for v in range(4):
                for q in range(2):
                    ref[0, v, q] = tile(0, v, q)
                ref[0, v, 2] = sums[0][0, v] + sums[1][0, v]

        @pl.when(k < 2)
        def _():
            put(a_keep)

        @pl.when(k >= 2)
        def _():
            put(a_away)
    else:
        a_all, b_all, a_over, b_over = outs
        for v in range(4):
            w = (0, 2, 1, 3)[v]
            a_all[0, v] = tile(0, v, 0)
            b_all[v, 0] = tile(1, v, 1)
            a_over[0, w] = tile(0, v, 1)
            b_over[w, 0] = tile(1, v, 0)


def gram(lefts, mean, right, at, sums, vmem):
    terms = len(lefts)
    high, low = right
    n = high.shape[1]
    h = high.shape[0] // 2
    g = n // 8
    specs = [pl.BlockSpec((1, 2 * g), lambda k, at: (0, at[k]))]
    args = [mean]
    for t, left in enumerate(lefts):
        specs.append(pl.BlockSpec((h, 2 * g), lambda k, at, t=t: (at[4 + 2 * t], at[k])))
        row = pl.BlockSpec(
            (h, n), lambda k, at, t=t: (at[5 + 2 * t], 0), pipeline_mode=pl.Buffered(1)
        )
        specs += [row, row]
        args += [left, high, low]
    in_row = pl.BlockSpec((1, 4, g, g), lambda k, at: (k, 0, 0, 0))
    in_col = pl.BlockSpec((4, 1, g, g), lambda k, at: (0, k, 0, 0))
    shapes = [(1, h)] * terms
    outs = [pl.BlockSpec((1, h), lambda k, at: (0, 0))] * terms
    if sums:
        specs += [in_row, in_row, in_col, in_col]
        args += sums
        shapes += [(2, 4, 3, g, g)] * 4
        outs += [
            pl.BlockSpec((1, 4, 3, g, g), lambda k, at: (jnp.minimum(k, 1), 0, 0, 0, 0)),
            pl.BlockSpec((1, 4, 3, g, g), lambda k, at: (jnp.maximum(k - 2, 0), 0, 0, 0, 0)),
        ] + [pl.BlockSpec((2, 1, 3, g, g), lambda k, at: (0, k, 0, 0, 0))] * 2
    else:
        shapes += [(4, 4, g, g)] * 4
        outs += [
            in_row,
            in_col,
            pl.BlockSpec((1, 4, g, g), lambda k, at: (swapped(k), 0, 0, 0)),
            pl.BlockSpec((4, 1, g, g), lambda k, at: (0, swapped(k), 0, 0)),
        ]
    res = pl.pallas_call(
        functools.partial(gram_body, terms=terms, extra=bool(sums)),
        grid_spec=pltpu.PrefetchScalarGridSpec(
            num_scalar_prefetch=1, grid=(4,), in_specs=specs, out_specs=outs
        ),
        out_shape=[jax.ShapeDtypeStruct(i, jnp.float32) for i in shapes],
        cost_estimate=pl.CostEstimate(
            flops=6 * terms * h * n * n, bytes_accessed=8 * n * n, transcendentals=0
        ),
        compiler_params=pltpu.CompilerParams(vmem_limit_bytes=vmem),
    )(at, *args)
    return res[:terms], res[terms:]


def flip_body(a_ref, out_ref):
    for i in range(a_ref.shape[0]):
        out_ref[i] = a_ref[i].T


def flip(a):
    return pl.pallas_call(
        flip_body,
        out_shape=jax.ShapeDtypeStruct(a.shape, jnp.float32),
        compiler_params=pltpu.CompilerParams(vmem_limit_bytes=VMEM),
        name="flip",
    )(a)


def combine_body(
    at_ref, pa, pb, qa, qb, got, p_own, p_other, q_left, q_right,
    norm0, norm1, near0, near1, far0, own_ref, out1, out2, out3, sums_ref, blocks,
    *, scenarios,
):
    c, e, h = at_ref[0], at_ref[1], at_ref[2]
    first = c == 0
    mine = lambda a, b: jnp.where(first, a, b)
    g = qa.shape[0]
    own = [mine(pa[i], pb[1 - i]) + p_own[i] for i in range(2)]
    other = [mine(got[1 - i], got[i]) + p_other[i] for i in range(2)]
    left = [
        mine(pa[2], pb[2]),
        mine(own[0], other[0]),
        mine(qa[...], qb[...]) + q_left[...],
        mine(other[0], own[0]),
    ]
    right = [
        got[2],
        mine(own[1], other[1]),
        got[3] + q_right[...],
        mine(other[1], own[1]),
    ]
    squares = None
    for i in range(4):
        for j, a in enumerate((left[i], right[i])):
            a = a * (1.0 / scenarios)
            blocks[i, :, j * g : (j + 1) * g] = a
            squares = a * a if squares is None else squares + a * a
    all_of = lambda a: jnp.sum(jnp.sum(a, axis=1, keepdims=True), axis=0, keepdims=True)
    frob = all_of(squares)
    n0, n1, m0, m1 = norm0[...], norm1[...], near0[...], near1[...]
    straight = n0 * m0 + n1 * m1
    crossed = n0 * m1 + n1 * m0
    far = jnp.where(h == 0, n0, n1) * far0[...]
    beta = all_of(n0 * n0 + n1 * n1 + 2.0 * (jnp.where(e == 0, straight, crossed) + far))
    trace = all_of(n0 + n1)
    lane = lax.broadcasted_iota(jnp.int32, (1, 128), 1)
    row = jnp.where(lane == 0, trace, jnp.where(lane == 1, beta, jnp.where(lane == 2, frob, 0.0)))
    sums_ref[...] = jnp.broadcast_to(row.reshape(1, 1, 128), sums_ref.shape)
    for i, ref in enumerate((own_ref, out1, out2, out3)):
        ref[...] = blocks[at_ref[3 + i]]


def combine(at, arrays, scenarios):
    g = arrays[2].shape[0]
    tile = jax.ShapeDtypeStruct((g, 2 * g), jnp.float32)
    return pl.pallas_call(
        functools.partial(combine_body, scenarios=scenarios),
        in_specs=[pl.BlockSpec(memory_space=pltpu.SMEM)]
        + [pl.BlockSpec(memory_space=pltpu.VMEM)] * len(arrays),
        out_shape=[tile] * 4 + [jax.ShapeDtypeStruct((128, 1, 128), jnp.float32)],
        scratch_shapes=[pltpu.VMEM((4, g, 2 * g), jnp.float32)],
        compiler_params=pltpu.CompilerParams(vmem_limit_bytes=VMEM),
        name="combine",
    )(at, *arrays)


def shrink_body(at_ref, own, got1, got2, got3, sums_ref, out_ref, *, scenarios, order):
    sums = jnp.sum(sums_ref[...], axis=0)
    lane = lax.broadcasted_iota(jnp.int32, sums.shape, 1)
    one = lambda i: jnp.sum(jnp.where(lane == i, sums, 0.0), axis=1, keepdims=True)
    trace_sum, beta_raw, frob_sum = one(0), one(1), one(2)
    target = trace_sum / (scenarios * order)
    beta_term = (beta_raw / scenarios - frob_sum) / (order * scenarios)
    delta_term = (frob_sum - order * target * target) / order
    shrinkage = beta_term / (delta_term + EPS)
    keep, add = 1.0 - shrinkage, shrinkage * target
    g, w = own.shape
    rows = lax.broadcasted_iota(jnp.int32, (g, w), 0)
    cols = lax.broadcasted_iota(jnp.int32, (g, w), 1)
    for i, ref in enumerate((own, got1, got2, got3)):
        at = at_ref[i]
        on = rows + at_ref[4] == cols + at * w
        to = pl.ds(pl.multiple_of(at * w, w), w)
        out_ref[:, to] = keep * ref[...] + jnp.where(on, add, 0.0)


def shrink(at, arrays, scenarios, order):
    g, w = arrays[0].shape
    return pl.pallas_call(
        functools.partial(shrink_body, scenarios=scenarios, order=order),
        in_specs=[pl.BlockSpec(memory_space=pltpu.SMEM)]
        + [pl.BlockSpec(memory_space=pltpu.VMEM)] * len(arrays),
        out_shape=jax.ShapeDtypeStruct((g, 4 * w), jnp.float32),
        compiler_params=pltpu.CompilerParams(vmem_limit_bytes=VMEM),
        name="shrink",
    )(at, *arrays)


def halve(keep, away, routes_of):
    got = send(away, routes_of[0])
    total = keep + got
    return total[0] + send(total[1], routes_of[1])


def finish(parts):
    a = halve(parts[0], parts[1], Y_HALF)
    b = halve(parts[2], parts[3], X_HALF)
    a = halve(a[:2], a[2:], X_HALF)
    return a, halve(b[:2], b[2:], Y_HALF)


def from_core(parts):
    return [send(parts[2 + i], OTHER_CORE) for i in range(2)]


def on_device(returns):
    local, n = returns.shape
    g = n // 8
    half = local // 2
    scenarios = local * 32
    order = n * 4
    x, y, c, z = (lax.axis_index(a) for a in AXES)
    first = c == 0
    low_z = (z < 2).astype(jnp.int32)
    early = lax.dynamic_slice_in_dim(returns, low_z * half, half)
    early, again = lax.optimization_barrier((early, returns))
    early_raw = send(early, TO_Z)
    late_raw = send(lax.dynamic_slice_in_dim(again, (1 - low_z) * half, half), TO_Z)
    far_raw = send(early_raw, TO_Z)
    sums = to_everyone(jnp.sum(returns, axis=0, keepdims=True), SCEN)
    mean = jnp.sum(sums, axis=0).reshape(1, n) / scenarios
    mean_near = send(mean, TO_Z)
    mean_far = send(mean, ACROSS)

    turn = [jnp.where(first, i, j) for i, j in ((0, 0), (3, 1), (1, 3), (2, 2))]
    ys = [y ^ i for i in turn]
    cols = [2 * (x ^ i) + k for i in turn for k in (c, 1 - c)]
    right = prepare(returns, mean, jnp.stack(cols))
    near_z = (z + jnp.where(first, 1, 3)) % 4
    near_early = (near_z < 2).astype(jnp.int32)
    far_half = 1 - low_z
    (norm0, norm1), d_parts = gram(
        [returns, returns], mean, right, jnp.stack(ys + [0, 0, 1, 1]), None, VMEM
    )
    d_over = from_core(d_parts)
    (near0, near1), p_parts = gram(
        [early_raw, late_raw],
        mean_near,
        right,
        jnp.stack(ys + [0, near_early, 0, 1 - near_early]),
        [d_parts[0], d_over[0], d_parts[1], d_over[1]],
        VMEM_LATE,
    )
    pa, pb = finish(p_parts)
    (far0,), q_parts = gram(
        [far_raw], mean_far, right, jnp.stack(ys + [0, far_half]), None, VMEM_LATE
    )
    q_over = from_core(q_parts)
    q_keep = [q_parts[i][:2] + q_over[i][:2] for i in range(2)]
    q_away = [q_parts[i][2:] + q_over[i][2:] for i in range(2)]
    q = finish([q_keep[0], q_away[0], q_keep[1], q_away[1]])

    mine = lambda a, b: jnp.where(first, a, b)
    p_flip = flip(jnp.stack([pa[0], pb[0], pa[1], pb[1]]))
    p_other = send(p_flip[:2], FLIP_NEAR[0])
    p_own = send(p_flip[2:], FLIP_NEAR[1])
    got = send(
        mine(jnp.concatenate([pb, q[1][None]]), jnp.concatenate([pa, q[0][None]])), OTHER_CORE
    )
    q_flip = flip(jnp.stack(q))
    q_left = send(q_flip[0], FLIP_FAR[0])
    q_right = send(q_flip[1], FLIP_FAR[1])
    at = jnp.stack([c, near_early, far_half] + [((x ^ i) - z) % 4 for i in range(4)])
    *tiles, sums = combine(
        at,
        [pa, pb, q[0], q[1], got, p_own, p_other, q_left, q_right]
        + [norm0, norm1, near0, near1, far0],
        scenarios,
    )
    tiles = [tiles[0]] + [send(tiles[i], X_BY[i]) for i in (1, 2, 3)]
    sums = lax.all_to_all(sums, AXES, split_axis=0, concat_axis=0, tiled=True)
    row = (x - z) * n + (2 * y + c) * g
    at = jnp.stack([x, x ^ 1, x ^ 2, x ^ 3, row])
    return shrink(at, tiles + [sums], scenarios, order)


def solution(mesh):
    torus = Mesh(mesh.devices.reshape(4, 4, 2, 4), AXES)
    spec = P(SCEN, "z")

    return jax.shard_map(on_device, mesh=torus, in_specs=(spec,), out_specs=spec, check_vma=False)
```
